256 devices in a mesh: pb: 32 (over z_hi, y, x), row: 8 (over z_lo, core).
Axes of the slice: x: 4, y: 4, z: 8 (z_hi: 2, z_lo: 4; z = z_hi * 4 + z_lo), core: 2. Of those that a mesh axis runs over, the one named last changes fastest.
Arguments:
- screened: bfloat16 [64, 2, 1024, 1024], P('pb', None, 'row'), may hold values from -1.0546875 to 1.0546875
- response: bfloat16 [64, 2, 1024, 1024], P(None, None, 'pb', 'row'), may hold values from -0.1875 to 0.1875
- q_owner: int32 [64], replicated, may hold values from 0 to 63, each once
- g_index: int32 [64, 1024], P('pb'), may hold values from 0 to 1023, each once within a row
Outputs:
- tangent: float32 [64, 2, 1024, 1024], P(None, None, ('row', 'pb'))
The draws below stay inside these ranges and needn't reach their ends.
Inputs may be any that keep to these rules, and one draw needn't show every extreme that they name: `q_owner`: each owner slot appears once. `g_index`: each row is a permutation of the 1024 plane waves.
All inputs are finite; a program needn't handle non-finite values.
Results may differ from the reference program's by a relative error of at most 0.0029.
Values may be sent and summed in bfloat16 or wider, within the bound.
No kernel may reach another device: no remote copies, remote signals or barrier semaphores. Data moves between devices by JAX's collectives and lax.ppermute only.
A program may use at most 64 MiB of HBM per device.

```python
import jax
import jax.numpy as jnp
from jax import lax

NG = 1024
Q = 64


def shard_levels(stream_key, shape, split, low, high):
    loudness = 1.0
    for axis_at, parts in split:
        heights = jax.random.uniform(jax.random.fold_in(jax.random.fold_in(stream_key, 6), axis_at), (parts,), jnp.float32, low / len(split), high / len(split))
        loudness = loudness * jnp.repeat(jnp.exp(heights), shape[axis_at] // parts).reshape((-1,) + (1,) * (len(shape) - 1 - axis_at))
    return loudness


def normal_values(own_key, shape, scale, reach, shards=(), kind=jnp.bfloat16):
    drawn = scale * jax.random.normal(own_key, shape, jnp.float32)
    if shards:
        drawn = drawn * shard_levels(own_key, shape, shards, -0.22, 0.18)
    return jnp.clip(drawn, -reach, reach).astype(kind)


def setup_inputs(seed: int = 0) -> dict:
    key_list = jax.random.split(jax.random.key(seed), 5)
    return {
        "screened": normal_values(key_list[0], (Q, 2, NG, NG), (NG ** -0.25), 1.0546875, ((0, 32), (2, 8))),
        "response": normal_values(key_list[1], (Q, 2, NG, NG), NG ** -0.5, 0.1875, ((2, 32), (3, 8))),
        "q_owner": jax.random.permutation(key_list[2], Q).astype(jnp.int32),
        "g_index": jax.vmap(lambda own: jax.random.permutation(own, NG))(jax.random.split(key_list[3], Q)).reshape((Q, NG)).astype(jnp.int32),
    }


def complex_product(left, right):
    real_part = jnp.dot(left[0], right[0], preferred_element_type=jnp.float32) - jnp.dot(left[1], right[1], preferred_element_type=jnp.float32)
    imag_part = jnp.dot(left[0], right[1], preferred_element_type=jnp.float32) + jnp.dot(left[1], right[0], preferred_element_type=jnp.float32)
    return jnp.stack((real_part, imag_part), axis=0)


def reference(screened, response, q_owner, g_index):
    inverse = jnp.zeros((Q,), jnp.int32).at[q_owner].set(jnp.arange(Q, dtype=jnp.int32))

    def one_slot(slot):
        source = inverse[slot]
        chi = response[source][:, g_index[slot], :]
        weight = screened[slot]
        halfway = complex_product(weight, chi).astype(jnp.bfloat16)
        return complex_product(halfway, weight)

    per_slot = lax.map(one_slot, jnp.arange(Q, dtype=jnp.int32))
    return jnp.take(per_slot, q_owner, axis=0)
```

```python
import jax
import jax.numpy as jnp
from jax import lax
from jax.sharding import Mesh, PartitionSpec as P

OWNER = ("zh", "y", "x")
ROW = ("zm", "zn", "c")
SPREAD = ("zh", "y", "x", "zm")


def swap(x, axes, mask=None):
    count = 2 ** len(axes)
    mask = count - 1 if mask is None else mask
    return lax.ppermute(x, axes, [(i, i ^ mask) for i in range(count)])


def complex_product(left, right):
    def product(first, second):
        return jnp.dot(first, second, preferred_element_type=jnp.float32)

    real_part = product(left[0], right[0]) - product(left[1], right[1])
    imag_part = product(left[0], right[1]) + product(left[1], right[0])
    return jnp.stack((real_part, imag_part))


def body(screened, response, q_owner, g_index):
    slots = q_owner.shape[0]
    _, parts, rows, size = screened.shape
    zm = lax.axis_index("zm")

    def pick(x, k, axis=0):
        return lax.dynamic_index_in_dim(x, k, axis, keepdims=False)

    mine = pick(screened, zm)
    other = swap(pick(screened, 1 - zm), ("zm",))
    pair = jnp.stack((mine, other))
    four = jnp.stack((pair, swap(pair, ("zn",))))
    whole = jnp.stack((four, swap(four, ("c",))))
    weight = jnp.moveaxis(whole, 3, 0).reshape(parts, size, size)

    ids = jnp.arange(slots, dtype=jnp.int32)
    inverse = jnp.sum(jnp.where(q_owner[None, :] == ids[:, None], ids[None, :], 0), axis=1)
    ordered = jnp.take(response, inverse, axis=0)
    landed = lax.all_to_all(ordered, SPREAD, 0, 0, tiled=True)
    short, columns = landed.shape[2:]
    landed = landed.reshape(slots // 2, 2, parts, short, columns)
    chi = jnp.stack((pick(landed, zm, 1), pick(landed, 1 - zm, 1)), axis=3)
    chi = jnp.moveaxis(chi, 1, 0).reshape(parts, size, 2 * columns)
    table = pick(g_index, zm)
    choose = (table[:, None] == jnp.arange(size, dtype=jnp.int32)[None, :]).astype(jnp.bfloat16)
    chi = jnp.einsum("ik,pkj->pij", choose, chi, preferred_element_type=jnp.float32)
    chi = chi.astype(jnp.bfloat16)

    half = complex_product(weight, chi).astype(jnp.bfloat16)
    blocks = half.reshape(parts, 2, 2, 2 * rows, 2 * columns)
    got = [
        blocks[:, 0, 0],
        swap(blocks[:, 0, 1], ("zn",)),
        swap(blocks[:, 1, 0], ("c",)),
        swap(blocks[:, 1, 1], ("zn", "c")),
    ]
    half = jnp.concatenate(got, axis=2)

    result = complex_product(half, weight).astype(jnp.bfloat16)
    own = slots // 2
    result = result.reshape(parts, 2, own, rows // own, size)
    result = jnp.stack((pick(result, zm, 1), pick(result, 1 - zm, 1)), axis=0)
    result = jnp.moveaxis(result, 2, 0)
    result = result.reshape(slots, parts, rows // own, size)
    returned = lax.all_to_all(result, SPREAD, 0, 0, tiled=True)
    return jnp.take(returned, q_owner, axis=0).astype(jnp.float32)


def solution(mesh):
    split = Mesh(mesh.devices.reshape(2, 4, 4, 2, 2, 2), OWNER + ROW)
    return jax.shard_map(
        body,
        mesh=split,
        in_specs=(P(OWNER, None, ROW, None), P(None, None, OWNER, ROW), P(), P(OWNER, None)),
        out_specs=P(None, None, ROW + OWNER, None),
        check_vma=False,
    )
```

```python
import jax
import jax.numpy as jnp
from jax import lax
from jax.experimental import pallas as pl
from jax.experimental.pallas import tpu as pltpu
from jax.sharding import Mesh, PartitionSpec as P

OWNER = ("zh", "y", "x")
ROW = ("zm", "zn", "c")
PLANE = ("y", "x")


def swap(x, axes, mask):
    count = 2 ** len(axes)
    return lax.ppermute(x, axes, [(i, i ^ mask) for i in range(count)])


def plane(x):
    return lax.all_to_all(x, PLANE, 0, 0, tiled=True)


def half_kernel(table_ref, *refs):
    w_refs, real_ref, imag_refs, outs = refs[:8], refs[8], refs[9:13], refs[13:17]
    w, chi, order, w_sems, chi_sems = refs[17:]
    width = real_ref.shape[-1]
    chi_copies, w_copies = [], []
    for ab in range(4):
        a, b = divmod(ab, 2)
        for part, source in ((0, real_ref.at[:, ab]), (1, imag_refs[ab])):
            lanes = pl.ds((part * 2 + b) * width, width)
            chi_copies.append(
                pltpu.make_async_copy(source, chi.at[a, :, :, lanes], chi_sems.at[2 * ab + part])
            )
    for k in range(8):
        w_copies.append(pltpu.make_async_copy(w_refs[k], w.at[k], w_sems.at[k]))
    for copy in chi_copies + w_copies:
        copy.start()
    size = order.shape[0]
    step = 128
    for i in range(0, size, step):
        ids = lax.broadcasted_iota(jnp.int32, (step, size), 1)
        hit = ids == table_ref[i : i + step, :]
        order[i : i + step, :] = jnp.where(hit, 1.0, 0.0).astype(jnp.bfloat16)
    for copy in chi_copies:
        copy.wait()
    both = chi[...].reshape(size, 4 * width)
    both = jnp.dot(order[...], both, preferred_element_type=jnp.float32)
    real, imag = both[:, : 2 * width], both[:, 2 * width :]
    first = both.astype(jnp.bfloat16)
    second = jnp.concatenate([-imag, real], axis=1).astype(jnp.bfloat16)
    for k in range(8):
        w_copies[k].wait()
        half = jnp.dot(w[k, 0], first, preferred_element_type=jnp.float32)
        half += jnp.dot(w[k, 1], second, preferred_element_type=jnp.float32)
        half = half.astype(jnp.bfloat16)
        dm, delta = k % 2, k // 2
        outs[delta][0, dm] = half[:, : 2 * width]
        outs[delta][1, dm] = half[:, 2 * width :]


def half_product(table, blocks, real, imags):
    rows, size = blocks[0].shape[1:]
    width = real.shape[-1]
    dense = pl.BlockSpec(memory_space=pltpu.VMEM)
    far = pl.BlockSpec(memory_space=pl.ANY)
    out = jax.ShapeDtypeStruct((2, 2, rows, 2 * width), jnp.bfloat16)
    return pl.pallas_call(
        half_kernel,
        out_shape=[out] * 4,
        in_specs=[dense] + [far] * 13,
        out_specs=[dense] * 4,
        scratch_shapes=[
            pltpu.VMEM((8, 2, rows, size), jnp.bfloat16),
            pltpu.VMEM((2, 16, size // 32, 4 * width), jnp.bfloat16),
            pltpu.VMEM((size, size), jnp.bfloat16),
            pltpu.SemaphoreType.DMA((8,)),
            pltpu.SemaphoreType.DMA((8,)),
        ],
        cost_estimate=pl.CostEstimate(
            flops=2 * size * size * 4 * width * 3, bytes_accessed=6 * 2**20, transcendentals=0
        ),
        name="half",
    )(table, *blocks, real, *imags)


def tangent_kernel(side_ref, *refs):
    w_refs, h_refs, outs = refs[:8], refs[8:12], refs[12:17]
    w, mixed, w_sems = refs[17:]
    rows = w.shape[2]
    copies = []
    for k in range(8):
        for part in range(2):
            copies.append(
                pltpu.make_async_copy(
                    w_refs[k].at[part], w.at[part, k], w_sems.at[2 * k + part]
                )
            )
    for copy in copies:
        copy.start()
    size = w.shape[3]
    left = jnp.concatenate(
        [h[...].reshape(4 * rows, 2 * rows) for h in h_refs], axis=1
    )
    for copy in copies:
        copy.wait()
    side = side_ref[0]
    wide = size // 2
    for h in range(2):
        lanes = slice(h * wide, h * wide + wide)
        by_real = jnp.dot(
            left, w[0, :, :, lanes].reshape(size, wide), preferred_element_type=jnp.float32
        )
        by_imag = jnp.dot(
            left, w[1, :, :, lanes].reshape(size, wide), preferred_element_type=jnp.float32
        )
        cut = 2 * rows
        real = by_real[:cut] - by_imag[cut:]
        imag = by_imag[:cut] + by_real[cut:]
        for j in range(2 * rows // 4):
            mixed[j, 0:4, :] = real[4 * j : 4 * j + 4, :]
            mixed[j, 4:8, :] = imag[4 * j : 4 * j + 4, :]
        for b in range(2):
            for high in range(2):
                a = high ^ side
                at = b * 32 + high * 16
                piece = mixed[at : at + 16].astype(jnp.bfloat16)
                if h == 1:
                    outs[4][a * 2 + b] = piece
                else:
                    @pl.when(a == 0)
                    def _():
                        outs[b][...] = piece

                    @pl.when(a == 1)
                    def _():
                        outs[2 + b][...] = piece


def tangent_product(side, blocks, halves):
    rows, size = blocks[0].shape[1:]
    dense = pl.BlockSpec(memory_space=pltpu.VMEM)
    far = pl.BlockSpec(memory_space=pl.ANY)
    piece = (16, 8, size // 2)
    return pl.pallas_call(
        tangent_kernel,
        out_shape=[jax.ShapeDtypeStruct(piece, jnp.bfloat16)] * 4
        + [jax.ShapeDtypeStruct((4,) + piece, jnp.bfloat16)],
        in_specs=[pl.BlockSpec(memory_space=pltpu.SMEM)] + [far] * 8 + [dense] * 4,
        out_specs=[dense] * 5,
        scratch_shapes=[
            pltpu.VMEM((2, 8, rows, size), jnp.bfloat16),
            pltpu.VMEM((2 * rows // 4, 8, size // 2), jnp.float32),
            pltpu.SemaphoreType.DMA((16,)),
        ],
        cost_estimate=pl.CostEstimate(
            flops=2 * 4 * rows * size * size * 2, bytes_accessed=6 * 2**20, transcendentals=0
        ),
        name="tangent",
    )(side, *blocks, *halves)


def body(screened, response, q_owner, g_index):
    slots = q_owner.shape[0]
    _, parts, rows, size = screened.shape
    zh, zm = lax.axis_index("zh"), lax.axis_index("zm")

    def pick(x, k, axis=0):
        return lax.dynamic_index_in_dim(x, k, axis, keepdims=False)

    def across(x, ab):
        return x if ab == 0 else swap(x, ("zh", "zm"), ab)

    ab = jnp.arange(4, dtype=jnp.int32)
    a, b = ab // 2, ab % 2
    slot = ((zh ^ a) * 32 + (zm ^ b))[:, None] + 2 * jnp.arange(16, dtype=jnp.int32)[None, :]
    ids = jnp.arange(slots, dtype=jnp.int32)

    def holder(slot):
        return jnp.sum(jnp.where(q_owner == slot[..., None], ids, 0), axis=-1)

    near = holder(slot)
    sent_real = [jnp.take(response[:, 0], near[k], axis=0) for k in range(4)]
    sent_imag = jnp.take(response[:, 1], holder(slot.T), axis=0)

    real = [across(sent_real[k], k) for k in range(4)]
    mine = pick(screened, zm)
    other = swap(pick(screened, 1 - zm), ("zm",), 1)
    imag = plane(sent_imag)
    imag = [across(imag[:, k], k) for k in range(4)]
    real = plane(jnp.stack(real, axis=1))

    blocks = [mine, other]
    blocks += [swap(block, ("zn",), 1) for block in blocks]
    blocks += [swap(block, ("c",), 1) for block in blocks]

    table = (pick(g_index, zm) ^ (zh * (size // 2)))[:, None]
    halves = half_product(table, blocks, real, imag)
    halves = [
        halves[0],
        swap(halves[1], ("zn",), 1),
        swap(halves[2], ("c",), 1),
        swap(halves[3], ("zn", "c"), 3),
    ]

    *fore, rest = tangent_product(zh[None].astype(jnp.int32), blocks, halves)
    fore = [across(fore[k], k) for k in range(4)]
    rest = plane(jnp.moveaxis(rest, 0, 1))
    rest = [across(rest[:, k], k) for k in range(4)]
    fore = plane(jnp.stack(fore, axis=1))
    rest = jnp.stack(rest, axis=1)

    q_yx, q_ab = (q_owner // 2) % 16, ((q_owner // 32) ^ zh) * 2 + ((q_owner % 2) ^ zm)
    found = q_yx * 4 + q_ab
    both = []
    for x in (fore, rest):
        x = jnp.take(x.reshape(slots, 2 * 4, size // 2), found, axis=0)
        both.append(x.reshape(slots, parts, 4, size // 2))
    return jnp.concatenate(both, axis=-1).astype(jnp.float32)


def solution(mesh):
    split = Mesh(mesh.devices.reshape(2, 4, 4, 2, 2, 2), OWNER + ROW)
    return jax.shard_map(
        body,
        mesh=split,
        in_specs=(P(OWNER, None, ROW, None), P(None, None, OWNER, ROW), P(), P(OWNER, None)),
        out_specs=P(None, None, ROW + OWNER, None),
        check_vma=False,
    )
```

```python
import jax
import jax.numpy as jnp
from jax import lax
from jax.experimental import pallas as pl
from jax.experimental.pallas import tpu as pltpu
from jax.sharding import Mesh, PartitionSpec as P

OWNER = ("zh", "y", "x")
ROW = ("zm", "zn", "c")
SPREAD = ("zh", "y", "x", "zm")


def swap(x, axes, mask):
    count = 2 ** len(axes)
    return lax.ppermute(x, axes, [(i, i ^ mask) for i in range(count)])


def spread(x):
    return lax.all_to_all(x, SPREAD, 0, 0, tiled=True)


def half_kernel(side_ref, table_ref, *refs):
    w_refs, landed_ref, outs = refs[:8], refs[8], refs[9:13]
    w, chi, order, w_sems, chi_sems = refs[13:]
    width = landed_ref.shape[-1]
    side = side_ref[0]
    chi_copies, w_copies = [], []
    for b in range(2):
        for part in range(2):
            at = part * 2 + b
            chi_copies.append(
                pltpu.make_async_copy(
                    landed_ref.at[:, side ^ b, part],
                    chi.at[:, :, pl.ds(at * width, width)],
                    chi_sems.at[at],
                )
            )
    for k in range(8):
        w_copies.append(pltpu.make_async_copy(w_refs[k], w.at[k], w_sems.at[k]))
    for copy in chi_copies + w_copies:
        copy.start()
    size = order.shape[0]
    step = 128
    for i in range(0, size, step):
        ids = lax.broadcasted_iota(jnp.int32, (step, size), 1)
        hit = ids == table_ref[i : i + step, :]
        order[i : i + step, :] = jnp.where(hit, 1.0, 0.0).astype(jnp.bfloat16)
    for copy in chi_copies:
        copy.wait()
    both = chi[...].reshape(size, 4 * width)
    both = jnp.dot(order[...], both, preferred_element_type=jnp.float32)
    real, imag = both[:, : 2 * width], both[:, 2 * width :]
    first = both.astype(jnp.bfloat16)
    second = jnp.concatenate([-imag, real], axis=1).astype(jnp.bfloat16)
    for k in range(8):
        w_copies[k].wait()
        half = jnp.dot(w[k, 0], first, preferred_element_type=jnp.float32)
        half += jnp.dot(w[k, 1], second, preferred_element_type=jnp.float32)
        half = half.astype(jnp.bfloat16)
        dm, delta = k % 2, k // 2
        outs[delta][0, dm] = half[:, : 2 * width]
        outs[delta][1, dm] = half[:, 2 * width :]


def half_product(side, table, blocks, landed):
    rows, size = blocks[0].shape[1:]
    owners, _, _, short, width = landed.shape
    dense = pl.BlockSpec(memory_space=pltpu.VMEM)
    far = pl.BlockSpec(memory_space=pl.ANY)
    out = jax.ShapeDtypeStruct((2, 2, rows, 2 * width), jnp.bfloat16)
    return pl.pallas_call(
        half_kernel,
        out_shape=[out] * 4,
        in_specs=[pl.BlockSpec(memory_space=pltpu.SMEM), dense] + [far] * 9,
        out_specs=[dense] * 4,
        scratch_shapes=[
            pltpu.VMEM((8, 2, rows, size), jnp.bfloat16),
            pltpu.VMEM((owners, short, 4 * width), jnp.bfloat16),
            pltpu.VMEM((size, size), jnp.bfloat16),
            pltpu.SemaphoreType.DMA((8,)),
            pltpu.SemaphoreType.DMA((4,)),
        ],
        cost_estimate=pl.CostEstimate(
            flops=2 * size * size * 4 * width * 3, bytes_accessed=6 * 2**20, transcendentals=0
        ),
        name="half",
    )(side, table, *blocks, landed)


def tangent_kernel(side_ref, *refs):
    w_refs, h_refs, out_ref = refs[:8], refs[8:12], refs[12]
    w, mixed, w_sems = refs[13:]
    rows = w.shape[2]
    copies = []
    for k in range(8):
        for part in range(2):
            copies.append(
                pltpu.make_async_copy(
                    w_refs[k].at[part], w.at[part, k], w_sems.at[2 * k + part]
                )
            )
    for copy in copies:
        copy.start()
    size = w.shape[3]
    left = jnp.concatenate(
        [h[...].reshape(4 * rows, 2 * rows) for h in h_refs], axis=1
    )
    for copy in copies:
        copy.wait()
    side = side_ref[0]
    wide = size // 2
    owners = out_ref.shape[0]
    for h in range(2):
        lanes = slice(h * wide, h * wide + wide)
        by_real = jnp.dot(
            left, w[0, :, :, lanes].reshape(size, wide), preferred_element_type=jnp.float32
        )
        by_imag = jnp.dot(
            left, w[1, :, :, lanes].reshape(size, wide), preferred_element_type=jnp.float32
        )
        cut = 2 * rows
        real = by_real[:cut] - by_imag[cut:]
        imag = by_imag[:cut] + by_real[cut:]
        for j in range(2 * owners):
            mixed[j, 0:4, :] = real[4 * j : 4 * j + 4, :]
            mixed[j, 4:8, :] = imag[4 * j : 4 * j + 4, :]
        for b in range(2):
            piece = mixed[b * owners : (b + 1) * owners].astype(jnp.bfloat16)
            out_ref[:, side ^ b, :, lanes] = piece


def tangent_product(side, blocks, halves):
    rows, size = blocks[0].shape[1:]
    owners = rows // 4
    dense = pl.BlockSpec(memory_space=pltpu.VMEM)
    far = pl.BlockSpec(memory_space=pl.ANY)
    return pl.pallas_call(
        tangent_kernel,
        out_shape=jax.ShapeDtypeStruct((owners, 2, 8, size), jnp.bfloat16),
        in_specs=[pl.BlockSpec(memory_space=pltpu.SMEM)] + [far] * 8 + [dense] * 4,
        out_specs=dense,
        scratch_shapes=[
            pltpu.VMEM((2, 8, rows, size), jnp.bfloat16),
            pltpu.VMEM((2 * owners, 8, size // 2), jnp.float32),
            pltpu.SemaphoreType.DMA((16,)),
        ],
        cost_estimate=pl.CostEstimate(
            flops=2 * 4 * rows * size * size * 2, bytes_accessed=6 * 2**20, transcendentals=0
        ),
        name="tangent",
    )(side, *blocks, *halves)


def body(screened, response, q_owner, g_index):
    slots = q_owner.shape[0]
    _, parts, rows, size = screened.shape
    short, width = response.shape[2:]
    zm = lax.axis_index("zm")
    side = zm[None].astype(jnp.int32)

    def pick(x, k):
        return lax.dynamic_index_in_dim(x, k, 0, keepdims=False)

    mine = pick(screened, zm)
    other = swap(pick(screened, 1 - zm), ("zm",), 1)

    ids = jnp.arange(slots, dtype=jnp.int32)
    inverse = jnp.sum(jnp.where(q_owner[None, :] == ids[:, None], ids[None, :], 0), axis=1)
    ordered = response.at[inverse].get(mode="promise_in_bounds")
    landed = spread(ordered).reshape(slots // 2, 2, parts, short, width)

    blocks = [mine, other]
    blocks += [swap(block, ("zn",), 1) for block in blocks]
    blocks += [swap(block, ("c",), 1) for block in blocks]

    halves = half_product(side, pick(g_index, zm)[:, None], blocks, landed)
    halves = [
        halves[0],
        swap(halves[1], ("zn",), 1),
        swap(halves[2], ("c",), 1),
        swap(halves[3], ("zn", "c"), 3),
    ]

    result = tangent_product(side, blocks, halves).reshape(slots, parts * 4, size)
    returned = spread(result)
    returned = returned.at[q_owner].get(mode="promise_in_bounds")
    return returned.reshape(slots, parts, 4, size).astype(jnp.float32)


def solution(mesh):
    split = Mesh(mesh.devices.reshape(2, 4, 4, 2, 2, 2), OWNER + ROW)
    return jax.shard_map(
        body,
        mesh=split,
        in_specs=(P(OWNER, None, ROW, None), P(None, None, OWNER, ROW), P(), P(OWNER, None)),
        out_specs=P(None, None, ROW + OWNER, None),
        check_vma=False,
    )
```

```python
import jax
import jax.numpy as jnp
from jax import lax
from jax.experimental import pallas as pl
from jax.experimental.pallas import tpu as pltpu
from jax.sharding import Mesh, PartitionSpec as P


OWNER = ("zh", "y", "x")
ROW = ("zm", "zn", "c")
SPREAD = ("zh", "y", "x", "zm")

FAR = pl.BlockSpec(memory_space=pltpu.MemorySpace.HBM)
DENSE = pl.BlockSpec(memory_space=pltpu.VMEM)
VMEM = pltpu.VMEM
PARAMS = pltpu.CompilerParams(vmem_limit_bytes=32 * 2**20)


def swap(x, axes, mask):
    count = 2 ** len(axes)
    return lax.ppermute(x, axes, [(i, i ^ mask) for i in range(count)])


def near(xs):
    return [pltpu.with_memory_space_constraint(x, pltpu.VMEM) for x in xs]


def far(xs):
    return [pltpu.with_memory_space_constraint(x, pltpu.MemorySpace.HBM) for x in xs]


def spread(x):
    return lax.all_to_all(x, SPREAD, 0, 0, tiled=True)


def order_kernel(side_ref, table_ref, out_ref):
    size = out_ref.shape[0]
    step = 128
    for i in range(0, size, step):
        ids = lax.broadcasted_iota(jnp.int32, (step, size), 1)
        hit = ids == table_ref[i : i + step, :]
        out_ref[i : i + step, :] = jnp.where(hit, 1.0, 0.0).astype(jnp.bfloat16)


def order_matrix(side, table):
    size = table.shape[0]
    return pl.pallas_call(
        order_kernel,
        out_shape=VMEM((size, size), jnp.bfloat16),
        in_specs=[pl.BlockSpec(memory_space=pltpu.SMEM), DENSE],
        out_specs=DENSE,
        compiler_params=PARAMS,
        name="order",
    )(side, table)


def half_kernel(side_ref, order_ref, landed_ref, *refs):
    w_refs, outs = refs[:8], refs[8:12]
    w, chi, w_sems, chi_sems = refs[12:]
    width = landed_ref.shape[-1]
    side = side_ref[0]
    chi_copies, w_copies = [], []
    for b in range(2):
        for part in range(2):
            at = part * 2 + b
            chi_copies.append(
                pltpu.make_async_copy(
                    landed_ref.at[:, side ^ b, part],
                    chi.at[:, :, pl.ds(at * width, width)],
                    chi_sems.at[at],
                )
            )
    for k in range(8):
        w_copies.append(pltpu.make_async_copy(w_refs[k], w.at[k], w_sems.at[k]))
    for copy in chi_copies + w_copies:
        copy.start()
    size = order_ref.shape[0]
    for copy in chi_copies:
        copy.wait()
    both = chi[...].reshape(size, 4 * width)
    both = jnp.dot(order_ref[...], both, preferred_element_type=jnp.float32)
    real, imag = both[:, : 2 * width], both[:, 2 * width :]
    first = both.astype(jnp.bfloat16)
    second = jnp.concatenate([-imag, real], axis=1).astype(jnp.bfloat16)
    for k in range(8):
        w_copies[k].wait()
        half = jnp.dot(w[k, 0], first, preferred_element_type=jnp.float32)
        half += jnp.dot(w[k, 1], second, preferred_element_type=jnp.float32)
        half = half.astype(jnp.bfloat16)
        dm, delta = k % 2, k // 2
        outs[delta][0, dm] = half[:, : 2 * width]
        outs[delta][1, dm] = half[:, 2 * width :]


def half_product(side, order, blocks, landed):
    rows, size = blocks[0].shape[1:]
    owners, _, _, short, width = landed.shape
    return pl.pallas_call(
        half_kernel,
        out_shape=[VMEM((2, 2, rows, 2 * width), jnp.bfloat16)] * 4,
        in_specs=[pl.BlockSpec(memory_space=pltpu.SMEM), DENSE] + [FAR] * 9,
        out_specs=[DENSE] * 4,
        scratch_shapes=[
            pltpu.VMEM((8, 2, rows, size), jnp.bfloat16),
            pltpu.VMEM((owners, short, 4 * width), jnp.bfloat16),
            pltpu.SemaphoreType.DMA((8,)),
            pltpu.SemaphoreType.DMA((4,)),
        ],
        compiler_params=PARAMS,
        cost_estimate=pl.CostEstimate(
            flops=2 * size * size * 4 * width * 3, bytes_accessed=6 * 2**20, transcendentals=0
        ),
        name="half",
    )(side, *near([order]), *far([landed, *blocks]))


def tangent_kernel(side_ref, *refs):
    w_refs, h_refs, out_ref = refs[:8], refs[8:12], refs[12]
    w, mixed, w_sems = refs[13:]
    rows, size = w.shape[2:]
    copies = []
    for k in range(8):
        for part in range(2):
            copies.append(
                pltpu.make_async_copy(
                    w_refs[k].at[part], w.at[part, k], w_sems.at[2 * k + part]
                )
            )
    for copy in copies:
        copy.start()
    left = jnp.concatenate([h[...].reshape(4 * rows, 2 * rows) for h in h_refs], axis=1)
    for copy in copies:
        copy.wait()
    side = side_ref[0]
    wide = size // 2
    owners = out_ref.shape[0]
    for h in range(2):
        lanes = slice(h * wide, h * wide + wide)

        def by(part):
            right = w[part, :, :, lanes].reshape(size, wide)
            return jnp.dot(left, right, preferred_element_type=jnp.float32)

        by_real, by_imag = by(0), by(1)
        cut = 2 * rows
        real = by_real[:cut] - by_imag[cut:]
        imag = by_imag[:cut] + by_real[cut:]
        for j in range(2 * owners):
            mixed[j, 0:4, :] = real[4 * j : 4 * j + 4, :]
            mixed[j, 4:8, :] = imag[4 * j : 4 * j + 4, :]
        for b in range(2):
            piece = mixed[b * owners : (b + 1) * owners].astype(jnp.bfloat16)
            out_ref[:, side ^ b, :, lanes] = piece


def tangent_product(side, blocks, halves):
    rows, size = blocks[0].shape[1:]
    owners = rows // 4
    return pl.pallas_call(
        tangent_kernel,
        out_shape=VMEM((owners, 2, 8, size), jnp.bfloat16),
        in_specs=[pl.BlockSpec(memory_space=pltpu.SMEM)] + [FAR] * 8 + [DENSE] * 4,
        out_specs=DENSE,
        scratch_shapes=[
            pltpu.VMEM((2, 8, rows, size), jnp.bfloat16),
            pltpu.VMEM((2 * owners, 8, size // 2), jnp.float32),
            pltpu.SemaphoreType.DMA((16,)),
        ],
        compiler_params=PARAMS,
        cost_estimate=pl.CostEstimate(
            flops=2 * 4 * rows * size * size * 2, bytes_accessed=6 * 2**20, transcendentals=0
        ),
        name="tangent",
    )(side, *far(blocks), *near(halves))


def steps(screened, response, q_owner, g_index):
    slots = q_owner.shape[0]
    _, parts, _, size = screened.shape
    short, width = response.shape[2:]
    zm = lax.axis_index("zm")
    side = zm[None].astype(jnp.int32)

    def pick(x, k):
        return lax.dynamic_index_in_dim(x, k, 0, keepdims=False)

    mine = pick(screened, zm)
    other = swap(pick(screened, 1 - zm), ("zm",), 1)
    across = [swap(mine, ("zn",), 1)]
    order = order_matrix(side, pick(g_index, zm)[:, None])

    ids = jnp.arange(slots, dtype=jnp.int32)
    inverse = jnp.sum(jnp.where(q_owner[None, :] == ids[:, None], ids[None, :], 0), axis=1)
    ordered = response.at[inverse].get(mode="promise_in_bounds")
    landed = spread(ordered)
    landed = landed.reshape(slots // 2, 2, parts, short, width)

    across.append(swap(other, ("zn",), 1))
    blocks = [mine, other] + across
    blocks += [swap(block, ("c",), 1) for block in blocks]

    halves = half_product(side, order, blocks, landed)
    halves = [
        halves[0],
        swap(halves[1], ("zn",), 1),
        swap(halves[2], ("c",), 1),
        swap(halves[3], ("zn", "c"), 3),
    ]

    result = tangent_product(side, blocks, halves).reshape(slots, parts * 4, size)
    returned = spread(result)
    returned = returned.at[q_owner].get(mode="promise_in_bounds")
    return returned.reshape(slots, parts, 4, size).astype(jnp.float32)


def solution(mesh):
    split = Mesh(mesh.devices.reshape(2, 4, 4, 2, 2, 2), OWNER + ROW)
    return jax.shard_map(
        steps,
        mesh=split,
        in_specs=(P(OWNER, None, ROW, None), P(None, None, OWNER, ROW), P(), P(OWNER, None)),
        out_specs=P(None, None, ROW + OWNER, None),
        check_vma=False,
    )
```

```python
import jax
import jax.numpy as jnp
from jax import lax
from jax.experimental import pallas as pl
from jax.experimental.pallas import tpu as pltpu
from jax.sharding import Mesh, PartitionSpec as P


OWNER = ("zh", "y", "x")
ROW = ("zm", "zn", "c")
SPREAD = ("zh", "y", "x", "zm")

FAR = pl.BlockSpec(memory_space=pltpu.MemorySpace.HBM)
DENSE = pl.BlockSpec(memory_space=pltpu.VMEM)
VMEM = pltpu.VMEM
PARAMS = pltpu.CompilerParams(vmem_limit_bytes=32 * 2**20)


def swap(x, axes, mask):
    count = 2 ** len(axes)
    return lax.ppermute(x, axes, [(i, i ^ mask) for i in range(count)])


def near(xs):
    return [pltpu.with_memory_space_constraint(x, pltpu.VMEM) for x in xs]


def far(xs):
    return [pltpu.with_memory_space_constraint(x, pltpu.MemorySpace.HBM) for x in xs]


def spread(x):
    return lax.all_to_all(x, SPREAD, 0, 0, tiled=True)


def order_kernel(side_ref, table_ref, out_ref):
    size = out_ref.shape[0]
    step = 128
    for i in range(0, size, step):
        ids = lax.broadcasted_iota(jnp.int32, (step, size), 1)
        hit = ids == table_ref[i : i + step, :]
        out_ref[i : i + step, :] = jnp.where(hit, 1.0, 0.0).astype(jnp.bfloat16)


def order_matrix(side, table):
    size = table.shape[0]
    return pl.pallas_call(
        order_kernel,
        out_shape=VMEM((size, size), jnp.bfloat16),
        in_specs=[pl.BlockSpec(memory_space=pltpu.SMEM), DENSE],
        out_specs=DENSE,
        compiler_params=PARAMS,
        name="order",
    )(side, table)


def half_block(w, k, both):
    width = both.shape[1] // 2
    real = jnp.dot(w[k, 0], both, preferred_element_type=jnp.float32)
    imag = jnp.dot(w[k, 1], both, preferred_element_type=jnp.float32)
    first = real[:, :width] - imag[:, width:]
    second = real[:, width:] + imag[:, :width]
    return first.astype(jnp.bfloat16), second.astype(jnp.bfloat16)


def early_kernel(side_ref, order_ref, landed_ref, *refs):
    w_refs, both_ref, own, cross, far_two, far_six = refs[:6], *refs[6:11]
    w, chi, w_sems, chi_sems = refs[11:]
    width = landed_ref.shape[-1]
    side = side_ref[0]
    chi_copies, w_copies = [], []
    for b in range(2):
        for part in range(2):
            at = part * 2 + b
            chi_copies.append(
                pltpu.make_async_copy(
                    landed_ref.at[:, side ^ b, part],
                    chi.at[:, :, pl.ds(at * width, width)],
                    chi_sems.at[at],
                )
            )
    for k in range(6):
        w_copies.append(pltpu.make_async_copy(w_refs[k], w.at[k], w_sems.at[k]))
    for copy in chi_copies + w_copies:
        copy.start()
    size = order_ref.shape[0]
    for copy in chi_copies:
        copy.wait()
    both = chi[...].reshape(size, 4 * width)
    both = jnp.dot(order_ref[...], both, preferred_element_type=jnp.float32)
    both = both.astype(jnp.bfloat16)
    both_ref[...] = both
    outs = (far_two, far_six, own.at[0], own.at[1], cross.at[0], cross.at[1])
    for k in range(6):
        w_copies[k].wait()
        outs[k][0], outs[k][1] = half_block(w, k, both)


def early_half(side, order, blocks, landed):
    rows, size = blocks[0].shape[1:]
    owners, _, _, short, width = landed.shape
    one = VMEM((2, rows, 2 * width), jnp.bfloat16)
    two = VMEM((2, 2, rows, 2 * width), jnp.bfloat16)
    return pl.pallas_call(
        early_kernel,
        out_shape=[VMEM((size, 4 * width), jnp.bfloat16), two, two, one, one],
        in_specs=[pl.BlockSpec(memory_space=pltpu.SMEM), DENSE] + [FAR] * 7,
        out_specs=[DENSE] * 5,
        scratch_shapes=[
            pltpu.VMEM((6, 2, rows, size), jnp.bfloat16),
            pltpu.VMEM((owners, short, 4 * width), jnp.bfloat16),
            pltpu.SemaphoreType.DMA((6,)),
            pltpu.SemaphoreType.DMA((4,)),
        ],
        compiler_params=PARAMS,
        cost_estimate=pl.CostEstimate(
            flops=5 * size * size * 4 * width, bytes_accessed=5 * 2**20, transcendentals=0
        ),
        name="early",
    )(side, *near([order]), *far([landed, *blocks]))


def late_kernel(both_ref, w_ref, v_ref, one_ref, two_ref, w, sems):
    copies = [
        pltpu.make_async_copy(ref, w.at[k], sems.at[k]) for k, ref in enumerate((w_ref, v_ref))
    ]
    for copy in copies:
        copy.start()
    for k, out in enumerate((one_ref, two_ref)):
        copies[k].wait()
        out[0], out[1] = half_block(w, k, both_ref[...])


def late_half(both, blocks):
    rows, size = blocks[0].shape[1:]
    one = VMEM((2, rows, both.shape[1] // 2), jnp.bfloat16)
    return pl.pallas_call(
        late_kernel,
        out_shape=[one, one],
        in_specs=[DENSE, FAR, FAR],
        out_specs=[DENSE] * 2,
        scratch_shapes=[
            pltpu.VMEM((2, 2, rows, size), jnp.bfloat16),
            pltpu.SemaphoreType.DMA((2,)),
        ],
        compiler_params=PARAMS,
        cost_estimate=pl.CostEstimate(
            flops=8 * rows * size * both.shape[1], bytes_accessed=2 * 2**20, transcendentals=0
        ),
        name="late",
    )(*near([both]), *far(blocks))


def tangent_kernel(side_ref, *refs):
    w_refs, h_refs, out_ref = refs[:8], refs[8:14], refs[14]
    w, mixed, w_sems = refs[15:]
    rows, size = w.shape[2:]
    copies = []
    for k in range(8):
        for part in range(2):
            copies.append(
                pltpu.make_async_copy(
                    w_refs[k].at[part], w.at[part, k], w_sems.at[2 * k + part]
                )
            )
    for copy in copies:
        copy.start()
    own, cross, *far_ones = h_refs
    pairs = ((own.at[0], own.at[1]), far_ones[:2], (cross.at[0], cross.at[1]), far_ones[2:])
    left = jnp.concatenate(
        [
            jnp.concatenate([h[part] for part in range(2) for h in pair], axis=0)
            for pair in pairs
        ],
        axis=1,
    )
    for copy in copies:
        copy.wait()
    side = side_ref[0]
    wide = size // 2
    owners = out_ref.shape[0]
    for h in range(2):
        lanes = slice(h * wide, h * wide + wide)

        def by(part):
            right = w[part, :, :, lanes].reshape(size, wide)
            return jnp.dot(left, right, preferred_element_type=jnp.float32)

        by_real, by_imag = by(0), by(1)
        cut = 2 * rows
        real = by_real[:cut] - by_imag[cut:]
        imag = by_imag[:cut] + by_real[cut:]
        for j in range(2 * owners):
            mixed[j, 0:4, :] = real[4 * j : 4 * j + 4, :]
            mixed[j, 4:8, :] = imag[4 * j : 4 * j + 4, :]
        for b in range(2):
            piece = mixed[b * owners : (b + 1) * owners].astype(jnp.bfloat16)
            out_ref[:, side ^ b, :, lanes] = piece


def tangent_product(side, blocks, halves):
    rows, size = blocks[0].shape[1:]
    owners = rows // 4
    return pl.pallas_call(
        tangent_kernel,
        out_shape=VMEM((owners, 2, 8, size), jnp.bfloat16),
        in_specs=[pl.BlockSpec(memory_space=pltpu.SMEM)] + [FAR] * 8 + [DENSE] * 6,
        out_specs=DENSE,
        scratch_shapes=[
            pltpu.VMEM((2, 8, rows, size), jnp.bfloat16),
            pltpu.VMEM((2 * owners, 8, size // 2), jnp.float32),
            pltpu.SemaphoreType.DMA((16,)),
        ],
        compiler_params=PARAMS,
        cost_estimate=pl.CostEstimate(
            flops=2 * 4 * rows * size * size * 2, bytes_accessed=6 * 2**20, transcendentals=0
        ),
        name="tangent",
    )(side, *far(blocks), *near(halves))


def steps(screened, response, q_owner, g_index):
    slots = q_owner.shape[0]
    _, parts, _, size = screened.shape
    short, width = response.shape[2:]
    zm = lax.axis_index("zm")
    side = zm[None].astype(jnp.int32)

    def pick(x, k):
        return lax.dynamic_index_in_dim(x, k, 0, keepdims=False)

    outgoing = pick(screened, 1 - zm)
    other = swap(outgoing, ("zm",), 1)
    screened, _ = lax.optimization_barrier((screened, outgoing))
    mine = pick(screened, zm)
    across = [swap(mine, ("zn",), 1)]
    order = order_matrix(side, pick(g_index, zm)[:, None])

    ids = jnp.arange(slots, dtype=jnp.int32)
    inverse = jnp.sum(jnp.where(q_owner[None, :] == ids[:, None], ids[None, :], 0), axis=1)
    ordered = response.at[inverse].get(mode="promise_in_bounds")
    landed = spread(ordered)
    landed = landed.reshape(slots // 2, 2, parts, short, width)

    across.append(swap(other, ("zn",), 1))
    blocks = [mine, other] + across
    blocks += [swap(block, ("c",), 1) for block in blocks[:3]]
    blocks.append(swap(blocks[3], ("c",), 1))

    ready = [blocks[k] for k in (2, 6, 0, 1, 4, 5)]
    both, own, cross, zn_first, far_first = early_half(side, order, ready, landed)
    zn_first = swap(zn_first, ("zn",), 1)
    far_first = swap(far_first, ("zn", "c"), 3)
    cross = swap(cross, ("c",), 1)
    zn_last, far_last = late_half(both, [blocks[3], blocks[7]])
    zn_last = swap(zn_last, ("zn",), 1)
    far_last = swap(far_last, ("zn", "c"), 3)
    halves = [own, cross, zn_first, zn_last, far_first, far_last]

    result = tangent_product(side, blocks, halves).reshape(slots, parts * 4, size)
    returned = spread(result)
    returned = returned.at[q_owner].get(mode="promise_in_bounds")
    return returned.reshape(slots, parts, 4, size).astype(jnp.float32)


def solution(mesh):
    split = Mesh(mesh.devices.reshape(2, 4, 4, 2, 2, 2), OWNER + ROW)
    return jax.shard_map(
        steps,
        mesh=split,
        in_specs=(P(OWNER, None, ROW, None), P(None, None, OWNER, ROW), P(), P(OWNER, None)),
        out_specs=P(None, None, ROW + OWNER, None),
        check_vma=False,
    )
```

```python
import jax
import jax.numpy as jnp
from jax import lax
from jax.experimental import pallas as pl
from jax.experimental.pallas import tpu as pltpu
from jax.sharding import Mesh, PartitionSpec as P


OWNER = ("zh", "y", "x")
ROW = ("zm", "zn", "c")
SPREAD = ("zh", "y", "x", "zm")

FAR = pl.BlockSpec(memory_space=pltpu.MemorySpace.HBM)
DENSE = pl.BlockSpec(memory_space=pltpu.VMEM)
VMEM = pltpu.VMEM
PARAMS = pltpu.CompilerParams(vmem_limit_bytes=32 * 2**20)


def swap(x, axes, mask):
    count = 2 ** len(axes)
    return lax.ppermute(x, axes, [(i, i ^ mask) for i in range(count)])


def near(xs):
    return [pltpu.with_memory_space_constraint(x, pltpu.VMEM) for x in xs]


def far(xs):
    return [pltpu.with_memory_space_constraint(x, pltpu.MemorySpace.HBM) for x in xs]


def spread(x):
    return lax.all_to_all(x, SPREAD, 0, 0, tiled=True)


def order_kernel(side_ref, table_ref, out_ref):
    size = out_ref.shape[0]
    step = 128
    for i in range(0, size, step):
        ids = lax.broadcasted_iota(jnp.int32, (step, size), 1)
        hit = ids == table_ref[i : i + step, :]
        out_ref[i : i + step, :] = jnp.where(hit, 1.0, 0.0).astype(jnp.bfloat16)


def order_matrix(side, table):
    size = table.shape[0]
    return pl.pallas_call(
        order_kernel,
        out_shape=VMEM((size, size), jnp.bfloat16),
        in_specs=[pl.BlockSpec(memory_space=pltpu.SMEM), DENSE],
        out_specs=DENSE,
        compiler_params=PARAMS,
        name="order",
    )(side, table)


def half_block(w, k, both):
    width = both.shape[1] // 2
    real = jnp.dot(w[0, k], both, preferred_element_type=jnp.float32)
    imag = jnp.dot(w[1, k], both, preferred_element_type=jnp.float32)
    first = real[:, :width] - imag[:, width:]
    second = real[:, width:] + imag[:, :width]
    return first.astype(jnp.bfloat16), second.astype(jnp.bfloat16)


def early_kernel(side_ref, order_ref, landed_ref, *refs):
    w_refs, both_ref, own, cross, w = refs[:4], *refs[4:8]
    chi, w_sems, chi_sems = refs[8:]
    width = landed_ref.shape[-1]
    side = side_ref[0]
    chi_copies, w_copies = [], []
    for b in range(2):
        for part in range(2):
            at = part * 2 + b
            chi_copies.append(
                pltpu.make_async_copy(
                    landed_ref.at[:, side ^ b, part],
                    chi.at[:, :, pl.ds(at * width, width)],
                    chi_sems.at[at],
                )
            )
    for k in range(4):
        w_copies.append(pltpu.make_async_copy(w_refs[k], w.at[:, k], w_sems.at[k]))
    for copy in chi_copies + w_copies:
        copy.start()
    size = order_ref.shape[0]
    for copy in chi_copies:
        copy.wait()
    both = chi[...].reshape(size, 4 * width)
    both = jnp.dot(order_ref[...], both, preferred_element_type=jnp.float32)
    both = both.astype(jnp.bfloat16)
    both_ref[...] = both
    outs = (own.at[0], own.at[1], cross.at[0], cross.at[1])
    for k in range(4):
        w_copies[k].wait()
        outs[k][0], outs[k][1] = half_block(w, k, both)


def early_half(side, order, blocks, landed):
    rows, size = blocks[0].shape[1:]
    owners, _, _, short, width = landed.shape
    two = VMEM((2, 2, rows, 2 * width), jnp.bfloat16)
    return pl.pallas_call(
        early_kernel,
        out_shape=[VMEM((size, 4 * width), jnp.bfloat16), two, two]
        + [VMEM((2, 4, rows, size), jnp.bfloat16)],
        in_specs=[pl.BlockSpec(memory_space=pltpu.SMEM), DENSE] + [FAR] * 5,
        out_specs=[DENSE] * 4,
        scratch_shapes=[
            pltpu.VMEM((owners, short, 4 * width), jnp.bfloat16),
            pltpu.SemaphoreType.DMA((4,)),
            pltpu.SemaphoreType.DMA((4,)),
        ],
        compiler_params=PARAMS,
        cost_estimate=pl.CostEstimate(
            flops=4 * size * size * 4 * width, bytes_accessed=5 * 2**20, transcendentals=0
        ),
        name="early",
    )(side, *near([order]), *far([landed, *blocks]))


def pair_kernel(both_ref, w_ref, v_ref, one_ref, two_ref, w, sems):
    copies = [
        pltpu.make_async_copy(ref, w.at[:, k], sems.at[k]) for k, ref in enumerate((w_ref, v_ref))
    ]
    for copy in copies:
        copy.start()
    for k, out in enumerate((one_ref, two_ref)):
        copies[k].wait()
        out[0], out[1] = half_block(w, k, both_ref[...])


def pair_half(both, blocks):
    rows, size = blocks[0].shape[1:]
    one = VMEM((2, rows, both.shape[1] // 2), jnp.bfloat16)
    return pl.pallas_call(
        pair_kernel,
        out_shape=[one, one, VMEM((2, 2, rows, size), jnp.bfloat16)],
        in_specs=[DENSE, FAR, DENSE],
        out_specs=[DENSE] * 3,
        scratch_shapes=[pltpu.SemaphoreType.DMA((2,))],
        compiler_params=PARAMS,
        cost_estimate=pl.CostEstimate(
            flops=8 * rows * size * both.shape[1], bytes_accessed=2 * 2**20, transcendentals=0
        ),
    )(*near([both]), *far(blocks[:1]), *near(blocks[1:]))


def tangent_kernel(side_ref, four, first_two, last_two, *refs):
    (own, cross, zn_first, zn_last, far_first, far_last), out_ref = refs[:6], refs[6]
    mixed = refs[7]
    rows, size = four.shape[2:]
    owners = out_ref.shape[0]
    wide = size // 2

    def stacked(first, last):
        return jnp.concatenate([h[part] for part in range(2) for h in (first, last)], axis=0)

    zn, distant = stacked(zn_first, zn_last), stacked(far_first, far_last)
    lefts = (
        jnp.concatenate([stacked(h.at[0], h.at[1]) for h in (own, cross)], axis=1),
        jnp.concatenate([zn[:, :rows], distant[:, :rows]], axis=1),
        jnp.concatenate([zn[:, rows:], distant[:, rows:]], axis=1),
    )
    for h in range(2):
        lanes = slice(h * wide, h * wide + wide)

        def by(part):
            total = 0.0
            for left, w in zip(lefts, (four, first_two, last_two)):
                right = w[part, :, :, lanes].reshape(left.shape[1], wide)
                total += jnp.dot(left, right, preferred_element_type=jnp.float32)
            return total

        by_real, by_imag = by(0), by(1)
        cut = 2 * rows
        real = by_real[:cut] - by_imag[cut:]
        imag = by_imag[:cut] + by_real[cut:]
        for j in range(2 * owners):
            mixed[j, 0:4, :] = real[4 * j : 4 * j + 4, :]
            mixed[j, 4:8, :] = imag[4 * j : 4 * j + 4, :]
        for b in range(2):
            piece = mixed[b * owners : (b + 1) * owners].astype(jnp.bfloat16)
            out_ref[:, side_ref[0] ^ b, :, lanes] = piece


def tangent_product(side, weights, halves):
    rows, size = weights[0].shape[2:]
    owners = rows // 4
    return pl.pallas_call(
        tangent_kernel,
        out_shape=jax.ShapeDtypeStruct((owners, 2, 8, size), jnp.bfloat16),
        in_specs=[pl.BlockSpec(memory_space=pltpu.SMEM)] + [DENSE] * 9,
        out_specs=DENSE,
        scratch_shapes=[pltpu.VMEM((2 * owners, 8, size // 2), jnp.float32)],
        compiler_params=PARAMS,
        cost_estimate=pl.CostEstimate(
            flops=2 * 4 * rows * size * size * 2, bytes_accessed=3 * 2**20, transcendentals=0
        ),
        name="tangent",
    )(side, *near([*weights, *halves]))


def steps(screened, response, q_owner, g_index):
    slots = q_owner.shape[0]
    _, parts, _, size = screened.shape
    short, width = response.shape[2:]
    zm = lax.axis_index("zm")
    side = zm[None].astype(jnp.int32)

    def pick(x, k):
        return lax.dynamic_index_in_dim(x, k, 0, keepdims=False)

    outgoing = pick(screened, 1 - zm)
    other = swap(outgoing, ("zm",), 1)
    screened, _ = lax.optimization_barrier((screened, outgoing))
    mine = pick(screened, zm)
    across = [swap(mine, ("zn",), 1)]
    order = order_matrix(side, pick(g_index, zm)[:, None])

    ids = jnp.arange(slots, dtype=jnp.int32)
    inverse = jnp.sum(jnp.where(q_owner[None, :] == ids[:, None], ids[None, :], 0), axis=1)
    ordered = response.at[inverse].get(mode="promise_in_bounds")
    landed = spread(ordered)
    landed = landed.reshape(slots // 2, 2, parts, short, width)

    across.append(swap(other, ("zn",), 1))
    blocks = [mine, other] + across
    blocks += [swap(block, ("c",), 1) for block in blocks[:2]]
    blocks.append(swap(blocks[2], ("c",), 1))
    blocks.append(swap(blocks[3], ("c",), 1))

    ready = [blocks[k] for k in (0, 1, 4, 5)]
    both, own, cross, four = early_half(side, order, ready, landed)
    zn_first, far_first, first_two = pair_half(both, [blocks[2], blocks[6]])
    zn_first = swap(zn_first, ("zn",), 1)
    far_first = swap(far_first, ("zn", "c"), 3)
    cross = swap(cross, ("c",), 1)
    zn_last, far_last, last_two = pair_half(both, [blocks[3], blocks[7]])
    zn_last = swap(zn_last, ("zn",), 1)
    far_last = swap(far_last, ("zn", "c"), 3)
    halves = [own, cross, zn_first, zn_last, far_first, far_last]

    result = tangent_product(side, (four, first_two, last_two), halves)
    returned = spread(result.reshape(slots, parts * 4, size))
    returned = returned.at[q_owner].get(mode="promise_in_bounds")
    return returned.reshape(slots, parts, 4, size).astype(jnp.float32)


def solution(mesh):
    split = Mesh(mesh.devices.reshape(2, 4, 4, 2, 2, 2), OWNER + ROW)
    return jax.shard_map(
        steps,
        mesh=split,
        in_specs=(P(OWNER, None, ROW, None), P(None, None, OWNER, ROW), P(), P(OWNER, None)),
        out_specs=P(None, None, ROW + OWNER, None),
        check_vma=False,
    )
```

```python
import jax
import jax.numpy as jnp
from jax import lax
from jax.experimental import pallas as pl
from jax.experimental.pallas import tpu as pltpu
from jax.sharding import Mesh, PartitionSpec as P


OWNER = ("zh", "y", "x")
ROW = ("zm", "zn", "c")
SPREAD = ("zh", "y", "x", "zm")

FAR = pl.BlockSpec(memory_space=pltpu.MemorySpace.HBM)
DENSE = pl.BlockSpec(memory_space=pltpu.VMEM)
VMEM = pltpu.VMEM
PARAMS = pltpu.CompilerParams(vmem_limit_bytes=32 * 2**20)


def swap(x, axes, mask):
    count = 2 ** len(axes)
    return lax.ppermute(x, axes, [(i, i ^ mask) for i in range(count)])


def near(xs):
    return [pltpu.with_memory_space_constraint(x, pltpu.VMEM) for x in xs]


def far(xs):
    return [pltpu.with_memory_space_constraint(x, pltpu.MemorySpace.HBM) for x in xs]


def spread(x):
    return lax.all_to_all(x, SPREAD, 0, 0, tiled=True)


def order_kernel(side_ref, table_ref, out_ref):
    size = out_ref.shape[0]
    step = 128
    for i in range(0, size, step):
        ids = lax.broadcasted_iota(jnp.int32, (step, size), 1)
        hit = ids == table_ref[i : i + step, :]
        out_ref[i : i + step, :] = jnp.where(hit, 1.0, 0.0).astype(jnp.bfloat16)


def order_matrix(side, table):
    size = table.shape[0]
    return pl.pallas_call(
        order_kernel,
        out_shape=VMEM((size, size), jnp.bfloat16),
        in_specs=[pl.BlockSpec(memory_space=pltpu.SMEM), DENSE],
        out_specs=DENSE,
        compiler_params=PARAMS,
        name="order",
    )(side, table)


def half_block(w, k, both):
    width = both.shape[1] // 2
    real = jnp.dot(w[0, k], both, preferred_element_type=jnp.float32)
    imag = jnp.dot(w[1, k], both, preferred_element_type=jnp.float32)
    first = real[:, :width] - imag[:, width:]
    second = real[:, width:] + imag[:, :width]
    return first.astype(jnp.bfloat16), second.astype(jnp.bfloat16)


def early_kernel(side_ref, order_ref, landed_ref, *refs):
    w_refs, both_ref, own, cross, far_two, far_six, w = refs[:6], *refs[6:12]
    chi, w_sems, chi_sems = refs[12:]
    width = landed_ref.shape[-1]
    side = side_ref[0]
    chi_copies, w_copies = [], []
    for b in range(2):
        for part in range(2):
            at = part * 2 + b
            chi_copies.append(
                pltpu.make_async_copy(
                    landed_ref.at[:, side ^ b, part],
                    chi.at[:, :, pl.ds(at * width, width)],
                    chi_sems.at[at],
                )
            )
    for k in range(6):
        w_copies.append(pltpu.make_async_copy(w_refs[k], w.at[:, k], w_sems.at[k]))
    for copy in chi_copies + w_copies:
        copy.start()
    size = order_ref.shape[0]
    for copy in chi_copies:
        copy.wait()
    both = chi[...].reshape(size, 4 * width)
    both = jnp.dot(order_ref[...], both, preferred_element_type=jnp.float32)
    both = both.astype(jnp.bfloat16)
    both_ref[...] = both
    outs = (own.at[0], own.at[1], cross.at[0], cross.at[1], far_two, far_six)
    for k in range(6):
        w_copies[k].wait()
        outs[k][0], outs[k][1] = half_block(w, k, both)


def early_half(side, order, blocks, landed):
    rows, size = blocks[0].shape[1:]
    owners, _, _, short, width = landed.shape
    one = VMEM((2, rows, 2 * width), jnp.bfloat16)
    two = VMEM((2, 2, rows, 2 * width), jnp.bfloat16)
    return pl.pallas_call(
        early_kernel,
        out_shape=[VMEM((size, 4 * width), jnp.bfloat16), two, two, one, one]
        + [VMEM((2, 6, rows, size), jnp.bfloat16)],
        in_specs=[pl.BlockSpec(memory_space=pltpu.SMEM), DENSE] + [FAR] * 7,
        out_specs=[DENSE] * 6,
        scratch_shapes=[
            pltpu.VMEM((owners, short, 4 * width), jnp.bfloat16),
            pltpu.SemaphoreType.DMA((6,)),
            pltpu.SemaphoreType.DMA((4,)),
        ],
        compiler_params=PARAMS,
        cost_estimate=pl.CostEstimate(
            flops=5 * size * size * 4 * width, bytes_accessed=5 * 2**20, transcendentals=0
        ),
        name="early",
    )(side, *near([order]), *far([landed, *blocks]))


def late_kernel(both_ref, w_ref, v_ref, one_ref, two_ref, w, sems):
    copies = [
        pltpu.make_async_copy(ref, w.at[:, k], sems.at[k]) for k, ref in enumerate((w_ref, v_ref))
    ]
    for copy in copies:
        copy.start()
    for k, out in enumerate((one_ref, two_ref)):
        copies[k].wait()
        out[0], out[1] = half_block(w, k, both_ref[...])


def late_half(both, blocks):
    rows, size = blocks[0].shape[1:]
    one = VMEM((2, rows, both.shape[1] // 2), jnp.bfloat16)
    return pl.pallas_call(
        late_kernel,
        out_shape=[one, one, VMEM((2, 2, rows, size), jnp.bfloat16)],
        in_specs=[DENSE, FAR, DENSE],
        out_specs=[DENSE] * 3,
        scratch_shapes=[pltpu.SemaphoreType.DMA((2,))],
        compiler_params=PARAMS,
        cost_estimate=pl.CostEstimate(
            flops=8 * rows * size * both.shape[1], bytes_accessed=2 * 2**20, transcendentals=0
        ),
        name="late",
    )(*near([both]), *far(blocks[:1]), *near(blocks[1:]))


def tangent_kernel(side_ref, six, two, *refs):
    (own, cross, zn_first, zn_last, far_first, far_last), out_ref = refs[:6], refs[6]
    mixed = refs[7]
    rows, size = six.shape[2:]
    owners = out_ref.shape[0]
    wide = size // 2

    def stacked(first, last):
        return jnp.concatenate([h[part] for part in range(2) for h in (first, last)], axis=0)

    zn, distant = stacked(zn_first, zn_last), stacked(far_first, far_last)
    inside = [stacked(h.at[0], h.at[1]) for h in (own, cross)]
    most = jnp.concatenate(inside + [zn[:, :rows], distant[:, :rows]], axis=1)
    rest = jnp.concatenate([zn[:, rows:], distant[:, rows:]], axis=1)
    for h in range(2):
        lanes = slice(h * wide, h * wide + wide)

        def by(part):
            total = 0.0
            for left, w in ((most, six), (rest, two)):
                right = w[part, :, :, lanes].reshape(left.shape[1], wide)
                total += jnp.dot(left, right, preferred_element_type=jnp.float32)
            return total

        by_real, by_imag = by(0), by(1)
        cut = 2 * rows
        real = by_real[:cut] - by_imag[cut:]
        imag = by_imag[:cut] + by_real[cut:]
        for j in range(2 * owners):
            mixed[j, 0:4, :] = real[4 * j : 4 * j + 4, :]
            mixed[j, 4:8, :] = imag[4 * j : 4 * j + 4, :]
        for b in range(2):
            piece = mixed[b * owners : (b + 1) * owners].astype(jnp.bfloat16)
            out_ref[:, side_ref[0] ^ b, :, lanes] = piece


def tangent_product(side, weights, halves):
    rows, size = weights[0].shape[2:]
    owners = rows // 4
    return pl.pallas_call(
        tangent_kernel,
        out_shape=jax.ShapeDtypeStruct((owners, 2, 8, size), jnp.bfloat16),
        in_specs=[pl.BlockSpec(memory_space=pltpu.SMEM)] + [DENSE] * 8,
        out_specs=DENSE,
        scratch_shapes=[pltpu.VMEM((2 * owners, 8, size // 2), jnp.float32)],
        compiler_params=PARAMS,
        cost_estimate=pl.CostEstimate(
            flops=2 * 4 * rows * size * size * 2, bytes_accessed=3 * 2**20, transcendentals=0
        ),
        name="tangent",
    )(side, *near([*weights, *halves]))


def steps(screened, response, q_owner, g_index):
    slots = q_owner.shape[0]
    _, parts, _, size = screened.shape
    short, width = response.shape[2:]
    zm = lax.axis_index("zm")
    side = zm[None].astype(jnp.int32)

    def pick(x, k):
        return lax.dynamic_index_in_dim(x, k, 0, keepdims=False)

    outgoing = pick(screened, 1 - zm)
    other = swap(outgoing, ("zm",), 1)
    screened, _ = lax.optimization_barrier((screened, outgoing))
    mine = pick(screened, zm)
    across = [swap(mine, ("zn",), 1)]
    order = order_matrix(side, pick(g_index, zm)[:, None])

    ids = jnp.arange(slots, dtype=jnp.int32)
    inverse = jnp.sum(jnp.where(q_owner[None, :] == ids[:, None], ids[None, :], 0), axis=1)
    ordered = response.at[inverse].get(mode="promise_in_bounds")
    landed = spread(ordered)
    landed = landed.reshape(slots // 2, 2, parts, short, width)

    across.append(swap(other, ("zn",), 1))
    blocks = [mine, other] + across
    blocks += [swap(block, ("c",), 1) for block in blocks[:3]]
    blocks.append(swap(blocks[3], ("c",), 1))

    ready = [blocks[k] for k in (0, 1, 4, 5, 2, 6)]
    both, own, cross, zn_first, far_first, six = early_half(side, order, ready, landed)
    zn_first = swap(zn_first, ("zn",), 1)
    far_first = swap(far_first, ("zn", "c"), 3)
    zn_last, far_last, two = late_half(both, [blocks[3], blocks[7]])
    zn_last = swap(zn_last, ("zn",), 1)
    far_last = swap(far_last, ("zn", "c"), 3)
    cross = swap(cross, ("c",), 1)
    halves = [own, cross, zn_first, zn_last, far_first, far_last]

    result = tangent_product(side, (six, two), halves)
    returned = spread(result.reshape(slots, parts * 4, size))
    returned = returned.at[q_owner].get(mode="promise_in_bounds")
    return returned.reshape(slots, parts, 4, size).astype(jnp.float32)


def solution(mesh):
    split = Mesh(mesh.devices.reshape(2, 4, 4, 2, 2, 2), OWNER + ROW)
    return jax.shard_map(
        steps,
        mesh=split,
        in_specs=(P(OWNER, None, ROW, None), P(None, None, OWNER, ROW), P(), P(OWNER, None)),
        out_specs=P(None, None, ROW + OWNER, None),
        check_vma=False,
    )
```

```python
import jax
import jax.numpy as jnp
from jax import lax
from jax.experimental import pallas as pl
from jax.experimental.pallas import tpu as pltpu
from jax.sharding import Mesh, PartitionSpec as P


OWNER = ("zh", "y", "x")
ROW = ("zm", "zn", "c")
SPREAD = ("zh", "y", "x", "zm")

FAR = pl.BlockSpec(memory_space=pltpu.MemorySpace.HBM)
DENSE = pl.BlockSpec(memory_space=pltpu.VMEM)
VMEM = pltpu.VMEM
PARAMS = pltpu.CompilerParams(vmem_limit_bytes=32 * 2**20)


def swap(x, axes, mask):
    count = 2 ** len(axes)
    return lax.ppermute(x, axes, [(i, i ^ mask) for i in range(count)])


def near(xs):
    return [pltpu.with_memory_space_constraint(x, pltpu.VMEM) for x in xs]


def far(xs):
    return [pltpu.with_memory_space_constraint(x, pltpu.MemorySpace.HBM) for x in xs]


def spread(x):
    return lax.all_to_all(x, SPREAD, 0, 0, tiled=True)


def order_kernel(side_ref, table_ref, out_ref):
    size = out_ref.shape[0]
    step = 128
    for i in range(0, size, step):
        ids = lax.broadcasted_iota(jnp.int32, (step, size), 1)
        hit = ids == table_ref[i : i + step, :]
        out_ref[i : i + step, :] = jnp.where(hit, 1.0, 0.0).astype(jnp.bfloat16)


def order_matrix(side, table):
    size = table.shape[0]
    return pl.pallas_call(
        order_kernel,
        out_shape=VMEM((size, size), jnp.bfloat16),
        in_specs=[pl.BlockSpec(memory_space=pltpu.SMEM), DENSE],
        out_specs=DENSE,
        compiler_params=PARAMS,
        name="order",
    )(side, table)


def half_block(w, k, both):
    width = both.shape[1] // 2
    real = jnp.dot(w[0, k], both, preferred_element_type=jnp.float32)
    imag = jnp.dot(w[1, k], both, preferred_element_type=jnp.float32)
    first = real[:, :width] - imag[:, width:]
    second = real[:, width:] + imag[:, :width]
    return first.astype(jnp.bfloat16), second.astype(jnp.bfloat16)


def early_kernel(side_ref, order_ref, landed_ref, *refs):
    w_refs, both_ref, one, two, w = refs[:2], *refs[2:6]
    chi, w_sems, chi_sems = refs[6:]
    width = landed_ref.shape[-1]
    side = side_ref[0]
    chi_copies, w_copies = [], []
    for b in range(2):
        for part in range(2):
            at = part * 2 + b
            chi_copies.append(
                pltpu.make_async_copy(
                    landed_ref.at[:, side ^ b, part],
                    chi.at[:, :, pl.ds(at * width, width)],
                    chi_sems.at[at],
                )
            )
    for k in range(2):
        w_copies.append(pltpu.make_async_copy(w_refs[k], w.at[:, k], w_sems.at[k]))
    for copy in chi_copies + w_copies:
        copy.start()
    size = order_ref.shape[0]
    for copy in chi_copies:
        copy.wait()
    both = chi[...].reshape(size, 4 * width)
    both = jnp.dot(order_ref[...], both, preferred_element_type=jnp.float32)
    both = both.astype(jnp.bfloat16)
    both_ref[...] = both
    outs = (one, two)
    for k in range(2):
        w_copies[k].wait()
        outs[k][0], outs[k][1] = half_block(w, k, both)


def early_half(side, order, blocks, landed):
    rows, size = blocks[0].shape[1:]
    owners, _, _, short, width = landed.shape
    one = VMEM((2, rows, 2 * width), jnp.bfloat16)
    return pl.pallas_call(
        early_kernel,
        out_shape=[VMEM((size, 4 * width), jnp.bfloat16), one, one]
        + [VMEM((2, 2, rows, size), jnp.bfloat16)],
        in_specs=[pl.BlockSpec(memory_space=pltpu.SMEM), DENSE] + [FAR] * 3,
        out_specs=[DENSE] * 4,
        scratch_shapes=[
            pltpu.VMEM((owners, short, 4 * width), jnp.bfloat16),
            pltpu.SemaphoreType.DMA((2,)),
            pltpu.SemaphoreType.DMA((4,)),
        ],
        compiler_params=PARAMS,
        cost_estimate=pl.CostEstimate(
            flops=3 * size * size * 4 * width, bytes_accessed=5 * 2**20, transcendentals=0
        ),
        name="early",
    )(side, *near([order]), *far([landed, *blocks]))


def pair_kernel(both_ref, w_ref, v_ref, one_ref, two_ref, w, sems):
    copies = [
        pltpu.make_async_copy(ref, w.at[:, k], sems.at[k]) for k, ref in enumerate((w_ref, v_ref))
    ]
    for copy in copies:
        copy.start()
    for k, out in enumerate((one_ref, two_ref)):
        copies[k].wait()
        out[0], out[1] = half_block(w, k, both_ref[...])


def pair_half(both, blocks):
    rows, size = blocks[0].shape[1:]
    one = VMEM((2, rows, both.shape[1] // 2), jnp.bfloat16)
    return pl.pallas_call(
        pair_kernel,
        out_shape=[one, one, VMEM((2, 2, rows, size), jnp.bfloat16)],
        in_specs=[DENSE, FAR, DENSE],
        out_specs=[DENSE] * 3,
        scratch_shapes=[pltpu.SemaphoreType.DMA((2,))],
        compiler_params=PARAMS,
        cost_estimate=pl.CostEstimate(
            flops=8 * rows * size * both.shape[1], bytes_accessed=2 * 2**20, transcendentals=0
        ),
    )(*near([both]), *far(blocks[:1]), *near(blocks[1:]))


def inside_kernel(both_ref, *refs):
    w_refs, own, cross, w, sems = refs[:4], *refs[4:8]
    copies = [
        pltpu.make_async_copy(ref, w.at[:, k], sems.at[k]) for k, ref in enumerate(w_refs)
    ]
    for copy in copies:
        copy.start()
    for k, out in enumerate((own.at[0], own.at[1], cross.at[0], cross.at[1])):
        copies[k].wait()
        out[0], out[1] = half_block(w, k, both_ref[...])


def inside_half(both, blocks):
    rows, size = blocks[0].shape[1:]
    two = VMEM((2, 2, rows, both.shape[1] // 2), jnp.bfloat16)
    return pl.pallas_call(
        inside_kernel,
        out_shape=[two, two, VMEM((2, 4, rows, size), jnp.bfloat16)],
        in_specs=[DENSE] + [FAR] * 4,
        out_specs=[DENSE] * 3,
        scratch_shapes=[pltpu.SemaphoreType.DMA((4,))],
        compiler_params=PARAMS,
        cost_estimate=pl.CostEstimate(
            flops=16 * rows * size * both.shape[1], bytes_accessed=4 * 2**20, transcendentals=0
        ),
        name="inside",
    )(*near([both]), *far(blocks))


def tangent_kernel(side_ref, four, first_two, last_two, *refs):
    (own, cross, zn_first, zn_last, far_first, far_last), out_ref = refs[:6], refs[6]
    mixed = refs[7]
    rows, size = four.shape[2:]
    owners = out_ref.shape[0]
    wide = size // 2

    def stacked(first, last):
        return jnp.concatenate([h[part] for part in range(2) for h in (first, last)], axis=0)

    zn, distant = stacked(zn_first, zn_last), stacked(far_first, far_last)
    lefts = (
        jnp.concatenate([stacked(h.at[0], h.at[1]) for h in (own, cross)], axis=1),
        jnp.concatenate([zn[:, :rows], distant[:, :rows]], axis=1),
        jnp.concatenate([zn[:, rows:], distant[:, rows:]], axis=1),
    )
    for h in range(2):
        lanes = slice(h * wide, h * wide + wide)

        def by(part):
            total = 0.0
            for left, w in zip(lefts, (four, first_two, last_two)):
                right = w[part, :, :, lanes].reshape(left.shape[1], wide)
                total += jnp.dot(left, right, preferred_element_type=jnp.float32)
            return total

        by_real, by_imag = by(0), by(1)
        cut = 2 * rows
        real = by_real[:cut] - by_imag[cut:]
        imag = by_imag[:cut] + by_real[cut:]
        for j in range(2 * owners):
            mixed[j, 0:4, :] = real[4 * j : 4 * j + 4, :]
            mixed[j, 4:8, :] = imag[4 * j : 4 * j + 4, :]
        for b in range(2):
            piece = mixed[b * owners : (b + 1) * owners].astype(jnp.bfloat16)
            out_ref[:, side_ref[0] ^ b, :, lanes] = piece


def tangent_product(side, weights, halves):
    rows, size = weights[0].shape[2:]
    owners = rows // 4
    return pl.pallas_call(
        tangent_kernel,
        out_shape=jax.ShapeDtypeStruct((owners, 2, 8, size), jnp.bfloat16),
        in_specs=[pl.BlockSpec(memory_space=pltpu.SMEM)] + [DENSE] * 9,
        out_specs=DENSE,
        scratch_shapes=[pltpu.VMEM((2 * owners, 8, size // 2), jnp.float32)],
        compiler_params=PARAMS,
        cost_estimate=pl.CostEstimate(
            flops=2 * 4 * rows * size * size * 2, bytes_accessed=3 * 2**20, transcendentals=0
        ),
        name="tangent",
    )(side, *near([*weights, *halves]))


def steps(screened, response, q_owner, g_index):
    slots = q_owner.shape[0]
    _, parts, _, size = screened.shape
    short, width = response.shape[2:]
    zm = lax.axis_index("zm")
    side = zm[None].astype(jnp.int32)

    def pick(x, k):
        return lax.dynamic_index_in_dim(x, k, 0, keepdims=False)

    outgoing = pick(screened, 1 - zm)
    other = swap(outgoing, ("zm",), 1)
    screened, _ = lax.optimization_barrier((screened, outgoing))
    mine = pick(screened, zm)
    across = [swap(mine, ("zn",), 1)]
    order = order_matrix(side, pick(g_index, zm)[:, None])

    ids = jnp.arange(slots, dtype=jnp.int32)
    inverse = jnp.sum(jnp.where(q_owner[None, :] == ids[:, None], ids[None, :], 0), axis=1)
    ordered = response.at[inverse].get(mode="promise_in_bounds")
    landed = spread(ordered)
    landed = landed.reshape(slots // 2, 2, parts, short, width)

    across.append(swap(other, ("zn",), 1))
    blocks = [mine, other] + across
    blocks += [swap(block, ("c",), 1) for block in blocks[:3]]
    blocks.append(swap(blocks[3], ("c",), 1))

    both, zn_first, far_first, first_two = early_half(side, order, [blocks[2], blocks[6]], landed)
    zn_first = swap(zn_first, ("zn",), 1)
    far_first = swap(far_first, ("zn", "c"), 3)
    zn_last, far_last, last_two = pair_half(both, [blocks[3], blocks[7]])
    zn_last = swap(zn_last, ("zn",), 1)
    far_last = swap(far_last, ("zn", "c"), 3)
    own, cross, four = inside_half(both, [blocks[k] for k in (0, 1, 4, 5)])
    cross = swap(cross, ("c",), 1)
    halves = [own, cross, zn_first, zn_last, far_first, far_last]

    result = tangent_product(side, (four, first_two, last_two), halves)
    returned = spread(result.reshape(slots, parts * 4, size))
    returned = returned.at[q_owner].get(mode="promise_in_bounds")
    return returned.reshape(slots, parts, 4, size).astype(jnp.float32)


def solution(mesh):
    split = Mesh(mesh.devices.reshape(2, 4, 4, 2, 2, 2), OWNER + ROW)
    return jax.shard_map(
        steps,
        mesh=split,
        in_specs=(P(OWNER, None, ROW, None), P(None, None, OWNER, ROW), P(), P(OWNER, None)),
        out_specs=P(None, None, ROW + OWNER, None),
        check_vma=False,
    )
```

```python
import jax
import jax.numpy as jnp
from jax import lax
from jax.experimental import pallas as pl
from jax.experimental.pallas import tpu as pltpu
from jax.sharding import Mesh, PartitionSpec as P


OWNER = ("zh", "y", "x")
ROW = ("zm", "zn", "c")
SPREAD = ("zh", "y", "x", "zm")

FAR = pl.BlockSpec(memory_space=pltpu.MemorySpace.HBM)
DENSE = pl.BlockSpec(memory_space=pltpu.VMEM)
VMEM = pltpu.VMEM
PARAMS = pltpu.CompilerParams(vmem_limit_bytes=32 * 2**20)


def swap(x, axes, mask):
    count = 2 ** len(axes)
    return lax.ppermute(x, axes, [(i, i ^ mask) for i in range(count)])


def near(xs):
    return [pltpu.with_memory_space_constraint(x, pltpu.VMEM) for x in xs]


def far(xs):
    return [pltpu.with_memory_space_constraint(x, pltpu.MemorySpace.HBM) for x in xs]


def spread(x):
    return lax.all_to_all(x, SPREAD, 0, 0, tiled=True)


def order_kernel(side_ref, table_ref, out_ref):
    size = out_ref.shape[0]
    step = 128
    for i in range(0, size, step):
        ids = lax.broadcasted_iota(jnp.int32, (step, size), 1)
        hit = ids == table_ref[i : i + step, :]
        out_ref[i : i + step, :] = jnp.where(hit, 1.0, 0.0).astype(jnp.bfloat16)


def order_matrix(side, table):
    size = table.shape[0]
    return pl.pallas_call(
        order_kernel,
        out_shape=VMEM((size, size), jnp.bfloat16),
        in_specs=[pl.BlockSpec(memory_space=pltpu.SMEM), DENSE],
        out_specs=DENSE,
        compiler_params=PARAMS,
        name="order",
    )(side, table)


def half_block(w, k, both):
    width = both.shape[1] // 2
    real = jnp.dot(w[0, k], both, preferred_element_type=jnp.float32)
    imag = jnp.dot(w[1, k], both, preferred_element_type=jnp.float32)
    first = real[:, :width] - imag[:, width:]
    second = real[:, width:] + imag[:, :width]
    return first.astype(jnp.bfloat16), second.astype(jnp.bfloat16)


def early_kernel(side_ref, order_ref, landed_ref, *refs):
    w_refs, both_ref, one, two, w = refs[:2], *refs[2:6]
    chi, w_sems, chi_sems = refs[6:]
    width = landed_ref.shape[-1]
    side = side_ref[0]
    chi_copies, w_copies = [], []
    for b in range(2):
        for part in range(2):
            at = part * 2 + b
            chi_copies.append(
                pltpu.make_async_copy(
                    landed_ref.at[:, side ^ b, part],
                    chi.at[:, :, pl.ds(at * width, width)],
                    chi_sems.at[at],
                )
            )
    for k in range(2):
        w_copies.append(pltpu.make_async_copy(w_refs[k], w.at[:, k], w_sems.at[k]))
    for copy in chi_copies + w_copies:
        copy.start()
    size = order_ref.shape[0]
    for copy in chi_copies:
        copy.wait()
    both = chi[...].reshape(size, 4 * width)
    both = jnp.dot(order_ref[...], both, preferred_element_type=jnp.float32)
    both = both.astype(jnp.bfloat16)
    both_ref[...] = both
    outs = (one, two)
    for k in range(2):
        w_copies[k].wait()
        outs[k][0], outs[k][1] = half_block(w, k, both)


def early_half(side, order, blocks, landed):
    rows, size = blocks[0].shape[1:]
    owners, _, _, short, width = landed.shape
    one = VMEM((2, rows, 2 * width), jnp.bfloat16)
    return pl.pallas_call(
        early_kernel,
        out_shape=[VMEM((size, 4 * width), jnp.bfloat16), one, one]
        + [VMEM((2, 2, rows, size), jnp.bfloat16)],
        in_specs=[pl.BlockSpec(memory_space=pltpu.SMEM), DENSE] + [FAR] * 3,
        out_specs=[DENSE] * 4,
        scratch_shapes=[
            pltpu.VMEM((owners, short, 4 * width), jnp.bfloat16),
            pltpu.SemaphoreType.DMA((2,)),
            pltpu.SemaphoreType.DMA((4,)),
        ],
        compiler_params=PARAMS,
        cost_estimate=pl.CostEstimate(
            flops=3 * size * size * 4 * width, bytes_accessed=5 * 2**20, transcendentals=0
        ),
        name="early",
    )(side, *near([order]), *far([landed, *blocks]))


def pair_kernel(both_ref, w_ref, v_ref, one_ref, two_ref, w, sems):
    copies = [
        pltpu.make_async_copy(ref, w.at[:, k], sems.at[k]) for k, ref in enumerate((w_ref, v_ref))
    ]
    for copy in copies:
        copy.start()
    for k, out in enumerate((one_ref, two_ref)):
        copies[k].wait()
        out[0], out[1] = half_block(w, k, both_ref[...])


def pair_half(both, blocks):
    rows, size = blocks[0].shape[1:]
    one = VMEM((2, rows, both.shape[1] // 2), jnp.bfloat16)
    return pl.pallas_call(
        pair_kernel,
        out_shape=[one, one, VMEM((2, 2, rows, size), jnp.bfloat16)],
        in_specs=[DENSE, FAR, DENSE],
        out_specs=[DENSE] * 3,
        scratch_shapes=[pltpu.SemaphoreType.DMA((2,))],
        compiler_params=PARAMS,
        cost_estimate=pl.CostEstimate(
            flops=8 * rows * size * both.shape[1], bytes_accessed=2 * 2**20, transcendentals=0
        ),
    )(*near([both]), *far(blocks[:1]), *near(blocks[1:]))


def inside_kernel(both_ref, *refs):
    w_refs, own, cross, w, sems = refs[:4], *refs[4:8]
    copies = [
        pltpu.make_async_copy(ref, w.at[:, k], sems.at[k]) for k, ref in enumerate(w_refs)
    ]
    for copy in copies:
        copy.start()
    for k, out in enumerate((own.at[0], own.at[1], cross.at[0], cross.at[1])):
        copies[k].wait()
        out[0], out[1] = half_block(w, k, both_ref[...])


def inside_half(both, blocks):
    rows, size = blocks[0].shape[1:]
    two = VMEM((2, 2, rows, both.shape[1] // 2), jnp.bfloat16)
    return pl.pallas_call(
        inside_kernel,
        out_shape=[two, two, VMEM((2, 4, rows, size), jnp.bfloat16)],
        in_specs=[DENSE] + [FAR] * 4,
        out_specs=[DENSE] * 3,
        scratch_shapes=[pltpu.SemaphoreType.DMA((4,))],
        compiler_params=PARAMS,
        cost_estimate=pl.CostEstimate(
            flops=16 * rows * size * both.shape[1], bytes_accessed=4 * 2**20, transcendentals=0
        ),
        name="inside",
    )(*near([both]), *far(blocks))


def tangent_kernel(side_ref, four, first_two, last_two, *refs):
    (own, cross, zn_first, zn_last, far_first, far_last), out_ref = refs[:6], refs[6]
    mixed = refs[7]
    rows, size = four.shape[2:]
    owners = out_ref.shape[0]
    wide = size // 2

    def stacked(first, last):
        return jnp.concatenate([h[part] for part in range(2) for h in (first, last)], axis=0)

    zn, distant = stacked(zn_first, zn_last), stacked(far_first, far_last)
    lefts = (
        jnp.concatenate([stacked(h.at[0], h.at[1]) for h in (own, cross)], axis=1),
        jnp.concatenate([zn[:, :rows], distant[:, :rows]], axis=1),
        jnp.concatenate([zn[:, rows:], distant[:, rows:]], axis=1),
    )
    for h in range(2):
        lanes = slice(h * wide, h * wide + wide)

        def by(part):
            total = 0.0
            for left, w in zip(lefts, (four, first_two, last_two)):
                right = w[part, :, :, lanes].reshape(left.shape[1], wide)
                total += jnp.dot(left, right, preferred_element_type=jnp.float32)
            return total

        by_real, by_imag = by(0), by(1)
        cut = 2 * rows
        real = by_real[:cut] - by_imag[cut:]
        imag = by_imag[:cut] + by_real[cut:]
        for j in range(2 * owners):
            mixed[j, 0:4, :] = real[4 * j : 4 * j + 4, :]
            mixed[j, 4:8, :] = imag[4 * j : 4 * j + 4, :]
        for b in range(2):
            piece = mixed[b * owners : (b + 1) * owners].astype(jnp.bfloat16)
            out_ref[:, side_ref[0] ^ b, :, lanes] = piece


def tangent_product(side, weights, halves):
    rows, size = weights[0].shape[2:]
    owners = rows // 4
    return pl.pallas_call(
        tangent_kernel,
        out_shape=jax.ShapeDtypeStruct((owners, 2, 8, size), jnp.bfloat16),
        in_specs=[pl.BlockSpec(memory_space=pltpu.SMEM)] + [DENSE] * 9,
        out_specs=DENSE,
        scratch_shapes=[pltpu.VMEM((2 * owners, 8, size // 2), jnp.float32)],
        compiler_params=PARAMS,
        cost_estimate=pl.CostEstimate(
            flops=2 * 4 * rows * size * size * 2, bytes_accessed=3 * 2**20, transcendentals=0
        ),
        name="tangent",
    )(side, *near([*weights, *halves]))


def order_back_kernel(owner_ref, found_ref, out_ref):
    count = out_ref.shape[0]
    base = pl.program_id(0) * count
    for j in range(count):
        value = found_ref[owner_ref[base + j]].astype(jnp.float32)
        out_ref[j, 0] = value[:4]
        out_ref[j, 1] = value[4:]


def order_back(q_owner, found):
    slots, _, size = found.shape
    return pl.pallas_call(
        order_back_kernel,
        grid=(4,),
        out_shape=jax.ShapeDtypeStruct((slots, 2, 4, size), jnp.float32),
        in_specs=[pl.BlockSpec(memory_space=pltpu.SMEM), DENSE],
        out_specs=pl.BlockSpec((slots // 4, 2, 4, size), lambda i: (i, 0, 0, 0)),
        compiler_params=PARAMS,
        name="order_back",
    )(q_owner, *near([found]))


def steps(screened, response, q_owner, g_index):
    slots = q_owner.shape[0]
    _, parts, _, size = screened.shape
    short, width = response.shape[2:]
    zm = lax.axis_index("zm")
    side = zm[None].astype(jnp.int32)

    def pick(x, k):
        return lax.dynamic_index_in_dim(x, k, 0, keepdims=False)

    outgoing = pick(screened, 1 - zm)
    other = swap(outgoing, ("zm",), 1)
    screened, _ = lax.optimization_barrier((screened, outgoing))
    mine = pick(screened, zm)
    across = [swap(mine, ("zn",), 1)]
    order = order_matrix(side, pick(g_index, zm)[:, None])

    ids = jnp.arange(slots, dtype=jnp.int32)
    inverse = jnp.sum(jnp.where(q_owner[None, :] == ids[:, None], ids[None, :], 0), axis=1)
    ordered = response.at[inverse].get(mode="promise_in_bounds")
    landed = spread(ordered)
    landed = landed.reshape(slots // 2, 2, parts, short, width)

    across.append(swap(other, ("zn",), 1))
    blocks = [mine, other] + across
    blocks += [swap(block, ("c",), 1) for block in blocks[:3]]
    blocks.append(swap(blocks[3], ("c",), 1))

    both, zn_first, far_first, first_two = early_half(side, order, [blocks[2], blocks[6]], landed)
    zn_first = swap(zn_first, ("zn",), 1)
    far_first = swap(far_first, ("zn", "c"), 3)
    zn_last, far_last, last_two = pair_half(both, [blocks[3], blocks[7]])
    zn_last = swap(zn_last, ("zn",), 1)
    far_last = swap(far_last, ("zn", "c"), 3)
    own, cross, four = inside_half(both, [blocks[k] for k in (0, 1, 4, 5)])
    cross = swap(cross, ("c",), 1)
    halves = [own, cross, zn_first, zn_last, far_first, far_last]

    result = tangent_product(side, (four, first_two, last_two), halves)
    returned = spread(result.reshape(slots, parts * 4, size))
    return order_back(q_owner, returned)


def solution(mesh):
    split = Mesh(mesh.devices.reshape(2, 4, 4, 2, 2, 2), OWNER + ROW)
    return jax.shard_map(
        steps,
        mesh=split,
        in_specs=(P(OWNER, None, ROW, None), P(None, None, OWNER, ROW), P(), P(OWNER, None)),
        out_specs=P(None, None, ROW + OWNER, None),
        check_vma=False,
    )
```
